32 devices in a mesh: dp: 4 (over y, core), vocab: 8 (over z, x).
Axes of the slice: x: 2, y: 2, z: 4, core: 2. Of those that a mesh axis runs over, the one named last changes fastest.
Arguments:
- latent_activations: bfloat16 [8, 448, 3584], P('dp', 'vocab'), as said below
- drawn_token_ids: int32 [8, 448], replicated, may hold values from 0 to 19455
- retained_ranking: int32 [4, 2], replicated, may hold values from 0 to 1, each once within a row
- unembedding_matrix: bfloat16 [3584, 19456], P('dp', 'vocab')
Outputs:
- logprob: float32 [4, 448], P('dp', 'vocab')
The draws below stay inside these ranges and needn't reach their ends.
Inputs may be any that keep to these rules, and one draw needn't show every extreme that they name: `retained_ranking`: each row is an ordering of the 2 candidates of one data group; its first 1 entries are the surviving sequences. `latent_activations`: final hidden states.
All inputs are finite; a program needn't handle non-finite values.
Results may differ from the reference program's by a relative error of at most 0.0003.
Values may be sent and summed in bfloat16 or wider, within the bound.
A program may use at most 128 MiB of HBM per device.

```python
import jax
import jax.numpy as jnp
from jax import lax

D = 3584
WIN = 448
RETAINED_SAMPLES = 1
BATCH_PROPOSALS = 2
CANDS = 8
VOCAB = 19456
N_DP = 4


def head_column(key, index):
    return 0.05 * jax.random.normal(jax.random.fold_in(key, index), (D,), jnp.float32)


def draw_unembedding_matrix(key, part):
    column_key = jax.random.fold_in(key, 11)
    columns = jax.vmap(lambda index: head_column(column_key, index))(jnp.arange(VOCAB, dtype=jnp.int32))
    return columns.T.astype(jnp.bfloat16)


def draw_latent_activations(key, part):
    shape = (CANDS, WIN, D)
    keys = jax.random.split(jax.random.fold_in(key, 23), 1)
    return jax.random.normal(keys[0], shape, jnp.float32).astype(jnp.bfloat16)


def touch_ends(array, own_key, low, top_value):
    extent = array.shape
    spot = [jax.random.randint(jax.random.fold_in(own_key, axis), (), 0, extent[axis]) for axis in range(len(extent))]
    array = array.at[tuple(spot)].set(low)
    longest = extent.index(max(extent))
    spot[longest] = (spot[longest] + 1) % extent[longest]
    return array.at[tuple(spot)].set(top_value)


def setup_inputs(seed: int = 0) -> dict:
    key_of = jax.random.split(jax.random.key(seed), 5)
    latent_activations = draw_latent_activations(jax.random.fold_in(key_of[4], 71), 0)
    drawn_token_ids = touch_ends(jax.random.randint(key_of[1], (CANDS, WIN), 0, VOCAB), jax.random.fold_in(key_of[1], 1), 0, VOCAB - 1).astype(jnp.int32)
    retained_ranking = jax.vmap(lambda own: jax.random.permutation(own, BATCH_PROPOSALS))(jax.random.split(key_of[2], N_DP)).reshape((N_DP, BATCH_PROPOSALS)).astype(jnp.int32)
    unembedding_matrix = draw_unembedding_matrix(jax.random.fold_in(key_of[4], 71), 0)
    return {"latent_activations": latent_activations, "drawn_token_ids": drawn_token_ids, "retained_ranking": retained_ranking, "unembedding_matrix": unembedding_matrix}


def reference(latent_activations, drawn_token_ids, retained_ranking, unembedding_matrix):
    prompt_clusters = jnp.arange(N_DP, dtype=jnp.int32)[:, None] * BATCH_PROPOSALS
    picked_samples = (retained_ranking[:, :RETAINED_SAMPLES] + prompt_clusters).reshape(-1).astype(jnp.int32)
    selected = latent_activations[picked_samples]
    chosen_ids = drawn_token_ids[picked_samples]

    def score_row(inputs):
        tokens, token_ids = inputs
        logits = jnp.dot(tokens, unembedding_matrix, preferred_element_type=jnp.float32)
        highest = jnp.max(logits, axis=1)
        totals = jnp.sum(jnp.exp(logits - highest[:, None]), axis=1)
        picked = jnp.take_along_axis(logits, token_ids[:, None], axis=1)[:, 0]
        return picked - (highest + jnp.log(totals))

    return lax.map(score_row, (selected, chosen_ids))
```

```python
import functools
import math

import jax
import jax.numpy as jnp
from jax import lax
from jax.experimental import pallas as pl
from jax.experimental.pallas import tpu as pltpu
from jax.sharding import PartitionSpec as P

BATCH_PROPOSALS = 2
MESH = pl.DeviceIdType.MESH
LANES = 128


class Plan:
    def __init__(self, n_dp, n_vocab, per_dev, width, depth):
        self.ny = n_dp // 2
        nx = math.isqrt(max(n_vocab // 2, 1))
        while n_vocab % nx:
            nx -= 1
        self.nx, self.nz = nx, n_vocab // nx
        self.n_dp, self.n_vocab = n_dp, n_vocab
        self.chips = self.ny * n_vocab
        self.per_dev = per_dev
        rows = 16
        while rows < per_dev:
            rows *= 2
        self.rows = rows
        self.tokens = self.chips * rows
        self.depth = depth
        tiles = width // LANES
        self.tiles = tiles
        self.own_tiles = -(-tiles // self.ny)
        self.cw = 2 * LANES if self.own_tiles % 2 == 0 else LANES
        self.cols = self.own_tiles * LANES
        self.chunks = self.cols // self.cw
        self.m_tile = min(512, self.tokens)

    def start(self, y):
        return jnp.minimum(y * self.own_tiles, self.tiles - self.own_tiles) * LANES


def flow_items(plan, order, flip):
    sizes = {"y": plan.ny, "x": plan.nx, "z": plan.nz}
    reach = {}
    for axis, n in sizes.items():
        far, near = n // 2, (n - 1) // 2
        reach[axis] = (near, far) if flip and axis == "z" else (far, near)
    items = []

    def visit(offset, last):
        sends = []
        for place, axis in enumerate(order):
            if place < last:
                continue
            plus, minus = reach[axis]
            at = offset.get(axis, 0)
            if at >= 0 and at < plus:
                sends.append((axis, 1))
            if at <= 0 and -at < minus:
                sends.append((axis, -1))
        items.append((dict(offset), sends))
        for axis, step in sends:
            moved = dict(offset)
            moved[axis] = moved.get(axis, 0) + step
            visit(moved, order.index(axis))

    visit({}, 0)
    items.sort(key=lambda item: sum(abs(v) for v in item[0].values()))
    return items


def kernel(plan, rank_ref, lat_ref, ids_ref, w_ref, out_ref, xbuf, wbuf, lg, m_ref, s_ref, p_ref, stats, got,
           x_send, x_recv, wl_sem, wy_send, wy_recv, wp_send, wp_recv, st_send, st_recv):
    ny, nx, nz, chips, rows = plan.ny, plan.nx, plan.nz, plan.chips, plan.rows
    dp, vocab = lax.axis_index("dp"), lax.axis_index("vocab")
    y, core = dp // 2, dp % 2
    z, x = vocab // nx, vocab % nx
    me = vocab * ny + y
    half = lat_ref.shape[2] // 2
    depth, cw = plan.depth, plan.cw

    def chip_device(b):
        return {"dp": (b % ny) * 2 + core, "vocab": b // ny}

    partner = {"dp": y * 2 + (1 - core), "vocab": vocab}

    base = pl.multiple_of(me * rows, rows)
    if rows != plan.per_dev:
        xbuf[pl.ds(base, rows), :] = jnp.zeros((rows, 2 * half), jnp.bfloat16)
    xbuf[pl.ds(base, plan.per_dev), :] = lat_ref[rank_ref[dp, 0]]

    barrier = pltpu.get_barrier_semaphore()

    @pl.loop(1, chips)
    def _(k):
        pl.semaphore_signal(barrier, inc=1, device_id=chip_device((me + k) % chips), device_id_type=MESH)

    pl.semaphore_signal(barrier, inc=1, device_id=partner, device_id_type=MESH)

    def w_rows(d):
        return pl.ds(pl.multiple_of(d * depth, depth), depth)

    def w_cols(j):
        return pl.ds(j * cw, cw)

    def window(y_at, j):
        return pl.ds(pl.multiple_of(plan.start(y_at) + j * cw, LANES), cw)

    locals_ = [
        pltpu.make_async_copy(w_ref.at[:, window(y, j)], wbuf.at[w_rows(dp), w_cols(j)], wl_sem.at[j])
        for j in range(plan.chunks)
    ]
    for copy in locals_:
        copy.start()
    pl.semaphore_wait(barrier, chips)

    def x_slice(flow, b):
        return xbuf.at[pl.ds(pl.multiple_of(b * rows, rows), rows), pl.ds(flow * half, half)]

    def origin(offset):
        oy = lax.rem(y - offset.get("y", 0) + ny, ny)
        ox = lax.rem(x - offset.get("x", 0) + nx, nx)
        oz = lax.rem(z - offset.get("z", 0) + nz, nz)
        return (oz * nx + ox) * ny + oy

    def x_copy(flow, b, axis, step):
        ty = lax.rem(y + (step if axis == "y" else 0) + ny, ny)
        tx = lax.rem(x + (step if axis == "x" else 0) + nx, nx)
        tz = lax.rem(z + (step if axis == "z" else 0) + nz, nz)
        return pltpu.make_async_remote_copy(
            src_ref=x_slice(flow, b), dst_ref=x_slice(flow, b), send_sem=x_send, recv_sem=x_recv.at[flow, b],
            device_id={"dp": ty * 2 + core, "vocab": tz * nx + tx}, device_id_type=MESH,
        )

    flows = (flow_items(plan, ("y", "x", "z"), False), flow_items(plan, ("y", "z", "x"), True))

    def wy_copy(k, j):
        y_to = lax.rem(y + k, ny)
        return pltpu.make_async_remote_copy(
            src_ref=w_ref.at[:, window(y_to, j)], dst_ref=wbuf.at[w_rows(dp), w_cols(j)],
            send_sem=wy_send.at[k, j], recv_sem=wy_recv.at[k, j],
            device_id={"dp": y_to * 2 + core, "vocab": vocab}, device_id_type=MESH,
        )

    def wp_copy(k, j):
        d = lax.rem(y - k + ny, ny) * 2 + core
        place = wbuf.at[w_rows(d), w_cols(j)]
        return pltpu.make_async_remote_copy(
            src_ref=w_ref.at[:, window(y, j)] if k == 0 else place, dst_ref=place,
            send_sem=wp_send.at[k, j], recv_sem=wp_recv.at[k, j],
            device_id=partner, device_id_type=MESH,
        )

    started = []
    for flow in range(2):
        offset, sends = flows[flow][0]
        for axis, step in sends:
            x_copy(flow, me, axis, step).start()
    for j in range(plan.chunks):
        for k in range(1, ny):
            copy = wy_copy(k, j)
            copy.start()
            started.append(copy)
    for j in range(plan.chunks):
        copy = wp_copy(0, j)
        copy.start()
        started.append(copy)

    def forward_w(j):
        for k in range(1, ny):
            wy_copy(k, j).wait_recv()
            copy = wp_copy(k, j)
            copy.start()
            started.append(copy)

    todo = [(flow, item) for pair in zip(flows[0][1:], flows[1][1:]) for flow, item in enumerate(pair)]
    due = 0
    for count, (flow, (offset, sends)) in enumerate(todo):
        b = origin(offset)
        x_copy(flow, b, "y", 0).wait_recv()
        for axis, step in sends:
            x_copy(flow, b, axis, step).start()
        while due < plan.chunks - 1 and (count + 1) * (plan.chunks - 0.5) >= (due + 2) * len(todo):
            forward_w(due)
            due += 1

    m_ref[...] = jnp.full(m_ref.shape, -jnp.inf, jnp.float32)
    s_ref[...] = jnp.zeros(s_ref.shape, jnp.float32)
    p_ref[...] = jnp.zeros(p_ref.shape, jnp.float32)
    lane = lax.broadcasted_iota(jnp.int32, (1, LANES), 1)
    repeated = y * plan.own_tiles * LANES - plan.start(y)
    for j in range(plan.chunks):
        while due < min(plan.chunks, j + 1):
            forward_w(due)
            due += 1
        locals_[j].wait()
        for k in range(ny):
            wp_copy(k, j).wait_recv()

        @pl.loop(0, plan.tokens // plan.m_tile)
        def _(i, j=j):
            top = pl.multiple_of(i * plan.m_tile, plan.m_tile)
            lg[...] = jnp.dot(
                xbuf[pl.ds(top, plan.m_tile), :], wbuf[:, w_cols(j)], preferred_element_type=jnp.float32
            )

            @pl.loop(0, plan.m_tile // 32, unroll=2)
            def _(r):
                here = pl.ds(pl.multiple_of(r * 32, 32), 32)
                there = pl.ds(pl.multiple_of(top + r * 32, 32), 32)
                parts = [lg[here, pl.ds(c * LANES, LANES)] for c in range(cw // LANES)]
                before = m_ref[there, :]
                now = before
                for part in parts:
                    now = jnp.maximum(now, part)
                total = s_ref[there, :] * jnp.exp(before - now)
                picked = p_ref[there, :]
                ids = ids_ref[there, :]
                for c, part in enumerate(parts):
                    first = j * cw + c * LANES
                    columns = lane + first
                    term = jnp.exp(part - now)
                    match = columns == ids
                    if first < (plan.own_tiles * ny - plan.tiles) * LANES:
                        own = columns >= repeated
                        term = jnp.where(own, term, 0.0)
                        match = jnp.logical_and(match, own)
                    total = total + term
                    picked = picked + jnp.where(match, part, 0.0)
                m_ref[there, :] = now
                s_ref[there, :] = total
                p_ref[there, :] = picked

    for g in range(plan.tokens // LANES):
        here = pl.ds(g * LANES, LANES)
        m = m_ref[here, :]
        top = jnp.max(m, axis=1, keepdims=True)
        total = jnp.sum(s_ref[here, :] * jnp.exp(m - top), axis=1, keepdims=True)
        picked = jnp.sum(p_ref[here, :], axis=1, keepdims=True)
        both = jnp.where(lane == 0, top, jnp.where(lane == 1, total, picked))
        stats[g] = both.T[:8, :]

    per_group = LANES // rows

    def st_copy(k):
        b = lax.rem(me + k, chips)
        return pltpu.make_async_remote_copy(
            src_ref=stats.at[b // per_group], dst_ref=got.at[k], send_sem=st_send, recv_sem=st_recv,
            device_id=chip_device(b), device_id_type=MESH,
        )

    @pl.loop(1, chips)
    def _(k):
        st_copy(k).start()

    got[0] = stats[me // per_group]
    for copy in started:
        copy.wait_send()
    sent = xbuf.at[pl.ds(0, (chips - 1) * rows), :]
    pltpu.make_async_copy(sent, sent, x_send).wait()
    others = got.at[pl.ds(1, chips - 1)]
    pltpu.make_async_copy(others, others, st_send).wait()
    pltpu.make_async_copy(others, others, st_recv).wait()
    top = got[0][0:1, :]
    for b in range(1, chips):
        top = jnp.maximum(top, got[b][0:1, :])
    total = jnp.zeros_like(top)
    picked = jnp.zeros_like(top)
    for b in range(chips):
        total = total + got[b][1:2, :] * jnp.exp(got[b][0:1, :] - top)
        picked = picked + got[b][2:3, :]
    result = picked - (top + jnp.log(total))
    place = lax.rem(me, per_group)
    value = result[:, : plan.per_dev]
    for c in range(1, per_group):
        value = jnp.where(place == c, result[:, c * rows : c * rows + plan.per_dev], value)
    out_ref[...] = value


def per_device(latent_activations, drawn_token_ids, retained_ranking, unembedding_matrix):
    depth, width = unembedding_matrix.shape
    n_dp, n_vocab = lax.axis_size("dp"), lax.axis_size("vocab")
    per_dev = latent_activations.shape[1]
    plan = Plan(n_dp, n_vocab, per_dev, width, depth)
    dp, vocab = lax.axis_index("dp"), lax.axis_index("vocab")
    ids = drawn_token_ids.reshape(n_dp, BATCH_PROPOSALS, n_vocab * per_dev)
    ids = jnp.where(retained_ranking[:, :1] == 0, ids[:, 0], ids[:, 1])
    ids = ids.reshape(plan.ny, 2, n_vocab, per_dev)
    ids = jnp.where(dp % 2 == 0, ids[:, 0], ids[:, 1]).transpose(1, 0, 2)
    ids = ids - (vocab * width + plan.start(dp // 2))
    ids = jnp.pad(ids, ((0, 0), (0, 0), (0, plan.rows - per_dev)), constant_values=-1)
    ids = ids.reshape(plan.tokens, 1)
    dma, vmem = pltpu.SemaphoreType.DMA, pltpu.VMEM
    model = depth * n_dp
    return pl.pallas_call(
        functools.partial(kernel, plan),
        out_shape=jax.ShapeDtypeStruct((1, per_dev), jnp.float32),
        in_specs=[
            pl.BlockSpec(memory_space=pltpu.SMEM),
            pl.BlockSpec(memory_space=vmem),
            pl.BlockSpec(memory_space=vmem),
            pl.BlockSpec(memory_space=pl.ANY),
        ],
        out_specs=pl.BlockSpec(memory_space=vmem),
        scratch_shapes=[
            vmem((plan.tokens, model), jnp.bfloat16),
            vmem((model, plan.cols), jnp.bfloat16),
            vmem((plan.m_tile, plan.cw), jnp.float32),
            vmem((plan.tokens, LANES), jnp.float32),
            vmem((plan.tokens, LANES), jnp.float32),
            vmem((plan.tokens, LANES), jnp.float32),
            vmem((plan.tokens // LANES, 8, LANES), jnp.float32),
            vmem((plan.chips, 8, LANES), jnp.float32),
            dma, dma((2, plan.chips)),
            dma((plan.chunks,)),
            dma((plan.ny, plan.chunks)), dma((plan.ny, plan.chunks)),
            dma((plan.ny, plan.chunks)), dma((plan.ny, plan.chunks)),
            dma, dma,
        ],
        compiler_params=pltpu.CompilerParams(
            collective_id=0, has_side_effects=True, vmem_limit_bytes=56 * 2**20
        ),
        name="score",
    )(retained_ranking, latent_activations, ids, unembedding_matrix)


def solution(mesh):
    return jax.shard_map(
        per_device,
        mesh=mesh,
        in_specs=(P("dp", "vocab", None), P(), P(), P("dp", "vocab")),
        out_specs=P("dp", "vocab"),
        check_vma=False,
    )
```

```python
import functools
import math

import jax
import jax.numpy as jnp
from jax import lax
from jax.experimental import pallas as pl
from jax.experimental.pallas import tpu as pltpu
from jax.sharding import PartitionSpec as P

BATCH_PROPOSALS = 2
MESH = pl.DeviceIdType.MESH
LANES = 128


class Plan:
    def __init__(self, n_dp, n_vocab, per_dev, width, depth):
        self.ny = n_dp // 2
        nx = math.isqrt(max(n_vocab // 2, 1))
        while n_vocab % nx:
            nx -= 1
        self.nx, self.nz = nx, n_vocab // nx
        self.n_dp, self.n_vocab = n_dp, n_vocab
        self.chips = self.ny * n_vocab
        self.per_dev = per_dev
        rows = 16
        while rows < per_dev:
            rows *= 2
        self.rows = rows
        self.tokens = self.chips * rows
        self.depth = depth
        tiles = width // LANES
        self.tiles = tiles
        self.own_tiles = -(-tiles // self.ny)
        self.cw = 2 * LANES if self.own_tiles % 2 == 0 else LANES
        self.cols = self.own_tiles * LANES
        self.chunks = self.cols // self.cw
        self.m_tile = self.nx * self.ny * rows
        self.sent_rows = per_dev if per_dev % 8 == 0 else rows

    def x_sends(self):
        ny, nx, nz = self.ny, self.nx, self.nz
        fan = {n: min(n - 1, 2) for n in (ny, nx, nz)}
        on = {n: int(n > 2) for n in (ny, nx, nz)}
        count = 2 * (fan[ny] + fan[nx] + fan[nz]) + 2 * (ny - 1) * (on[ny] + fan[nx] + fan[nz])
        count += (nx - 1) * ny * (on[nx] + fan[nz]) + (nz - 1) * nx * ny * on[nz]
        return count + (nz - 1) * ny * (on[nz] + fan[nx]) + nz * (nx - 1) * ny * on[nx]

    def start(self, y):
        return jnp.minimum(y * self.own_tiles, self.tiles - self.own_tiles) * LANES


def source(at, n, k):
    both = jnp.minimum(at, n - 1 - at)
    reach = (k + 1) // 2
    paired = at - reach if k % 2 else at + reach
    far = k - both
    single = jnp.where(at + at < n - 1, at + far, at - far)
    return jnp.where(k <= 2 * both, paired, single)


def kernel(plan, rank_ref, lat_ref, ids_ref, w_ref, out_ref, xbuf, wbuf, lg, m_ref, s_ref, p_ref, stats, got,
           x_send, x_recv, wl_sem, wy_send, wy_recv, wp_send, wp_recv, st_send, st_recv):
    ny, nx, nz, chips, rows = plan.ny, plan.nx, plan.nz, plan.chips, plan.rows
    dp, vocab = lax.axis_index("dp"), lax.axis_index("vocab")
    y, core = dp // 2, dp % 2
    z, x = vocab // nx, vocab % nx
    me = vocab * ny + y
    model = lat_ref.shape[2]
    first_width = max(model // LANES // 7, 1) * LANES
    depth, cw = plan.depth, plan.cw

    def chip_device(b):
        return {"dp": (b % ny) * 2 + core, "vocab": b // ny}

    partner = {"dp": y * 2 + (1 - core), "vocab": vocab}

    base = pl.multiple_of(me * rows, rows)
    if rows != plan.per_dev:
        xbuf[pl.ds(base, rows), :] = jnp.zeros((rows, model), jnp.bfloat16)
    xbuf[pl.ds(base, plan.per_dev), :] = lat_ref[rank_ref[dp, 0]]

    barrier = pltpu.get_barrier_semaphore()

    @pl.loop(1, chips)
    def _(k):
        pl.semaphore_signal(barrier, inc=1, device_id=chip_device((me + k) % chips), device_id_type=MESH)

    pl.semaphore_signal(barrier, inc=1, device_id=partner, device_id_type=MESH)

    def w_rows(d):
        return pl.ds(pl.multiple_of(d * depth, depth), depth)

    def w_cols(j):
        return pl.ds(j * cw, cw)

    def window(y_at, j):
        return pl.ds(pl.multiple_of(plan.start(y_at) + j * cw, LANES), cw)

    locals_ = [
        pltpu.make_async_copy(w_ref.at[:, window(y, j)], wbuf.at[w_rows(dp), w_cols(j)], wl_sem.at[j])
        for j in range(plan.chunks)
    ]
    for copy in locals_:
        copy.start()
    pl.semaphore_wait(barrier, chips)

    def x_slice(flow, b):
        cols = pl.ds(0, first_width) if flow == 0 else pl.ds(first_width, model - first_width)
        return xbuf.at[pl.ds(pl.multiple_of(b * rows, rows), plan.sent_rows), cols]

    def chip(iy, ix, iz):
        return (iz * nx + ix) * ny + iy

    spot = {"y": (y, ny), "x": (x, nx), "z": (z, nz)}

    sends = []

    def x_copy(flow, b, axis, step, slot):
        to = {name: at for name, (at, _) in spot.items()}
        to[axis] = to[axis] + step
        return pltpu.make_async_remote_copy(
            src_ref=x_slice(flow, b), dst_ref=x_slice(flow, b), send_sem=x_send.at[slot], recv_sem=x_recv.at[flow, b],
            device_id={"dp": to["y"] * 2 + core, "vocab": to["z"] * nx + to["x"]}, device_id_type=MESH,
        )

    def send(flow, b, axis, step, here):
        copy = x_copy(flow, b, axis, step, len(sends))
        sends.append((copy, here))
        if here is None:
            copy.start()
        else:
            pl.when(here)(copy.start)

    def spread(flow, b, axis):
        at, n = spot[axis]
        if n == 2:
            send(flow, b, axis, 1 - 2 * at, None)
        elif n > 2:
            send(flow, b, axis, 1, at + 1 < n)
            send(flow, b, axis, -1, at > 0)

    def onward(flow, b, axis, origin):
        at, n = spot[axis]
        if n > 2:
            step = jnp.where(origin < at, 1, -1)
            send(flow, b, axis, step, jnp.logical_and(at + step >= 0, at + step < n))

    def arrived(flow, b):
        x_copy(flow, b, "y", 0, 0).wait_recv()

    def wy_copy(k, j):
        y_to = lax.rem(y + k, ny)
        return pltpu.make_async_remote_copy(
            src_ref=w_ref.at[:, window(y_to, j)], dst_ref=wbuf.at[w_rows(dp), w_cols(j)],
            send_sem=wy_send.at[k, j], recv_sem=wy_recv.at[k, j],
            device_id={"dp": y_to * 2 + core, "vocab": vocab}, device_id_type=MESH,
        )

    def wp_copy(k, j):
        d = lax.rem(y - k + ny, ny) * 2 + core
        place = wbuf.at[w_rows(d), w_cols(j)]
        return pltpu.make_async_remote_copy(
            src_ref=w_ref.at[:, window(y, j)] if k == 0 else place, dst_ref=place,
            send_sem=wp_send.at[k, j], recv_sem=wp_recv.at[k, j],
            device_id=partner, device_id_type=MESH,
        )

    started = []
    for axis in ("y", "x", "z"):
        for flow in (1, 0):
            spread(flow, me, axis)
    for j in range(plan.chunks):
        for k in range(1, ny):
            copy = wy_copy(k, j)
            copy.start()
            started.append(copy)
    for j in range(plan.chunks):
        copy = wp_copy(0, j)
        copy.start()
        started.append(copy)

    def forward_w(j):
        for k in range(1, ny):
            wy_copy(k, j).wait_recv()
            copy = wp_copy(k, j)
            copy.start()
            started.append(copy)

    src = {
        axis: [spot[axis][0]] + [source(*spot[axis], k) for k in range(1, spot[axis][1])] for axis in spot
    }

    def y_items():
        for iy in src["y"][1:]:
            for flow in (1, 0):
                b = chip(iy, x, z)
                arrived(flow, b)
                onward(flow, b, "y", iy)
                for axis in ("x", "z"):
                    spread(flow, b, axis)

    def first_x_items():
        for ix in src["x"][1:]:
            for iy in src["y"]:
                b = chip(iy, ix, z)
                arrived(0, b)
                onward(0, b, "x", ix)
                spread(0, b, "z")

    def first_z_items(k):
        iz = src["z"][k]
        for ix in src["x"]:
            for iy in src["y"]:
                b = chip(iy, ix, iz)
                arrived(0, b)
                onward(0, b, "z", iz)

    def second_z_items(k):
        iz = src["z"][k]
        for iy in src["y"]:
            b = chip(iy, x, iz)
            arrived(1, b)
            onward(1, b, "z", iz)
            spread(1, b, "x")

    def second_x_items(k):
        iz = src["z"][k]
        for ix in src["x"][1:]:
            for iy in src["y"]:
                b = chip(iy, ix, iz)
                arrived(1, b)
                onward(1, b, "x", ix)

    lane = lax.broadcasted_iota(jnp.int32, (1, LANES), 1)
    repeated = y * plan.own_tiles * LANES - plan.start(y)
    m_tile = plan.m_tile

    def score(k, low, high):
        top = pl.multiple_of(src["z"][k] * m_tile, m_tile)

        @pl.loop(low, high)
        def _(j):
            start = pl.multiple_of(j * cw, cw)
            lg[...] = jnp.dot(
                xbuf[pl.ds(top, m_tile), :], wbuf[:, pl.ds(start, cw)], preferred_element_type=jnp.float32
            )
            columns = [lane + (start + c * LANES) for c in range(cw // LANES)]
            own = [at >= repeated for at in columns]
            columns = [jnp.where(mine, at, -(2**30)) for mine, at in zip(own, columns)]

            @pl.loop(0, m_tile // 32, unroll=2)
            def _(r):
                here = pl.ds(pl.multiple_of(r * 32, 32), 32)
                there = pl.ds(pl.multiple_of(top + r * 32, 32), 32)
                parts = [lg[here, pl.ds(c * LANES, LANES)] for c in range(cw // LANES)]
                before = m_ref[there, :]
                now = before
                for part in parts:
                    now = jnp.maximum(now, part)
                total = s_ref[there, :] * jnp.exp(before - now)
                picked = p_ref[there, :]
                ids = ids_ref[there, :]
                for c, part in enumerate(parts):
                    total = total + jnp.where(own[c], jnp.exp(part - now), 0.0)
                    picked = picked + jnp.where(columns[c] == ids, part, 0.0)
                m_ref[there, :] = now
                s_ref[there, :] = total
                p_ref[there, :] = picked

    def w_ready(j):
        forward_w(j)
        locals_[j].wait()
        for k in range(ny):
            wp_copy(k, j).wait_recv()

    m_ref[...] = jnp.full(m_ref.shape, -jnp.inf, jnp.float32)
    s_ref[...] = jnp.zeros(s_ref.shape, jnp.float32)
    p_ref[...] = jnp.zeros(p_ref.shape, jnp.float32)
    y_items()
    first_x_items()
    if nz > 1:
        second_z_items(1)
    second_x_items(0)
    done_w = 0
    for k in range(1, nz):
        if k + 1 < nz:
            second_z_items(k + 1)
        first_z_items(k)
        second_x_items(k)
        if k == nz - 1:
            break
        until = plan.chunks * (k + 1) // nz
        for j in range(done_w, until):
            w_ready(j)
        for t in range(k):
            score(t, done_w, until)
        score(k, 0, until)
        done_w = until
    for j in range(done_w, plan.chunks):
        w_ready(j)
    for t in range(nz - 1):
        score(t, done_w, plan.chunks)
    score(nz - 1, 0, plan.chunks)

    for g in range(plan.tokens // LANES):
        here = pl.ds(g * LANES, LANES)
        m = m_ref[here, :]
        top = jnp.max(m, axis=1, keepdims=True)
        total = jnp.sum(s_ref[here, :] * jnp.exp(m - top), axis=1, keepdims=True)
        picked = jnp.sum(p_ref[here, :], axis=1, keepdims=True)
        both = jnp.where(lane == 0, top, jnp.where(lane == 1, total, picked))
        stats[g] = both.T[:8, :]

    per_group = LANES // rows

    def st_copy(k):
        b = lax.rem(me + k, chips)
        return pltpu.make_async_remote_copy(
            src_ref=stats.at[b // per_group], dst_ref=got.at[k], send_sem=st_send, recv_sem=st_recv,
            device_id=chip_device(b), device_id_type=MESH,
        )

    @pl.loop(1, chips)
    def _(k):
        st_copy(k).start()

    got[0] = stats[me // per_group]
    for copy in started:
        copy.wait_send()
    for copy, here in sends:
        if here is None:
            copy.wait_send()
        else:
            pl.when(here)(copy.wait_send)
    others = got.at[pl.ds(1, chips - 1)]
    pltpu.make_async_copy(others, others, st_send).wait()
    pltpu.make_async_copy(others, others, st_recv).wait()
    top = got[0][0:1, :]
    for b in range(1, chips):
        top = jnp.maximum(top, got[b][0:1, :])
    total = jnp.zeros_like(top)
    picked = jnp.zeros_like(top)
    for b in range(chips):
        total = total + got[b][1:2, :] * jnp.exp(got[b][0:1, :] - top)
        picked = picked + got[b][2:3, :]
    result = picked - (top + jnp.log(total))
    place = lax.rem(me, per_group)
    value = result[:, : plan.per_dev]
    for c in range(1, per_group):
        value = jnp.where(place == c, result[:, c * rows : c * rows + plan.per_dev], value)
    out_ref[...] = value


def per_device(latent_activations, drawn_token_ids, retained_ranking, unembedding_matrix):
    depth, width = unembedding_matrix.shape
    n_dp, n_vocab = lax.axis_size("dp"), lax.axis_size("vocab")
    per_dev = latent_activations.shape[1]
    plan = Plan(n_dp, n_vocab, per_dev, width, depth)
    dp, vocab = lax.axis_index("dp"), lax.axis_index("vocab")
    ids = drawn_token_ids.reshape(n_dp, BATCH_PROPOSALS, n_vocab * per_dev)
    ids = jnp.where(retained_ranking[:, :1] == 0, ids[:, 0], ids[:, 1])
    ids = ids.reshape(plan.ny, 2, n_vocab, per_dev)
    ids = jnp.where(dp % 2 == 0, ids[:, 0], ids[:, 1]).transpose(1, 0, 2)
    ids = ids - (vocab * width + plan.start(dp // 2))
    ids = jnp.pad(ids, ((0, 0), (0, 0), (0, plan.rows - per_dev)), constant_values=-1)
    ids = ids.reshape(plan.tokens, 1)
    dma, vmem = pltpu.SemaphoreType.DMA, pltpu.VMEM
    model = depth * n_dp
    return pl.pallas_call(
        functools.partial(kernel, plan),
        out_shape=jax.ShapeDtypeStruct((1, per_dev), jnp.float32),
        in_specs=[
            pl.BlockSpec(memory_space=pltpu.SMEM),
            pl.BlockSpec(memory_space=vmem),
            pl.BlockSpec(memory_space=vmem),
            pl.BlockSpec(memory_space=pl.ANY),
        ],
        out_specs=pl.BlockSpec(memory_space=vmem),
        scratch_shapes=[
            vmem((plan.tokens, model), jnp.bfloat16),
            vmem((model, plan.cols), jnp.bfloat16),
            vmem((plan.m_tile, plan.cw), jnp.float32),
            vmem((plan.tokens, LANES), jnp.float32),
            vmem((plan.tokens, LANES), jnp.float32),
            vmem((plan.tokens, LANES), jnp.float32),
            vmem((plan.tokens // LANES, 8, LANES), jnp.float32),
            vmem((plan.chips, 8, LANES), jnp.float32),
            dma((plan.x_sends(),)), dma((2, plan.chips)),
            dma((plan.chunks,)),
            dma((plan.ny, plan.chunks)), dma((plan.ny, plan.chunks)),
            dma((plan.ny, plan.chunks)), dma((plan.ny, plan.chunks)),
            dma, dma,
        ],
        compiler_params=pltpu.CompilerParams(
            collective_id=0, has_side_effects=True, vmem_limit_bytes=56 * 2**20
        ),
        name="score",
    )(retained_ranking, latent_activations, ids, unembedding_matrix)


def solution(mesh):
    return jax.shard_map(
        per_device,
        mesh=mesh,
        in_specs=(P("dp", "vocab", None), P(), P(), P("dp", "vocab")),
        out_specs=P("dp", "vocab"),
        check_vma=False,
    )
```

```python
import functools
import math

import jax
import jax.numpy as jnp
from jax import lax
from jax.experimental import pallas as pl
from jax.experimental.pallas import tpu as pltpu
from jax.sharding import PartitionSpec as P

BATCH_PROPOSALS = 2
MESH = pl.DeviceIdType.MESH
LANES = 128


class Plan:
    def __init__(self, n_dp, n_vocab, per_dev, width, depth):
        self.ny = n_dp // 2
        nx = math.isqrt(max(n_vocab // 2, 1))
        while n_vocab % nx:
            nx -= 1
        self.nx, self.nz = nx, n_vocab // nx
        self.n_dp, self.n_vocab = n_dp, n_vocab
        self.chips = self.ny * n_vocab
        self.per_dev = per_dev
        rows = 16
        while rows < per_dev:
            rows *= 2
        self.rows = rows
        self.tokens = self.chips * rows
        self.depth = depth
        tiles = width // LANES
        self.tiles = tiles
        self.own_tiles = -(-tiles // self.ny)
        self.cw = 2 * LANES if self.own_tiles % 2 == 0 else LANES
        self.cols = self.own_tiles * LANES
        self.chunks = self.cols // self.cw
        self.m_tile = self.nx * self.ny * rows
        self.sent_rows = per_dev if per_dev % 8 == 0 else rows

    def x_sends(self):
        ny, nx, nz = self.ny, self.nx, self.nz
        fan = {n: min(n - 1, 2) for n in (ny, nx, nz)}
        on = {n: int(n > 2) for n in (ny, nx, nz)}
        count = 2 * (fan[ny] + fan[nx] + fan[nz]) + 2 * (ny - 1) * (on[ny] + fan[nx] + fan[nz])
        count += (nx - 1) * ny * (on[nx] + fan[nz]) + (nz - 1) * nx * ny * on[nz]
        return count + (nz - 1) * ny * (on[nz] + fan[nx]) + nz * (nx - 1) * ny * on[nx]

    def start(self, y):
        return jnp.minimum(y * self.own_tiles, self.tiles - self.own_tiles) * LANES


def source(at, n, k):
    both = jnp.minimum(at, n - 1 - at)
    reach = (k + 1) // 2
    paired = at - reach if k % 2 else at + reach
    far = k - both
    single = jnp.where(at + at < n - 1, at + far, at - far)
    return jnp.where(k <= 2 * both, paired, single)


def kernel(plan, rank_ref, lat_ref, ids_ref, w_ref, out_ref, xbuf, wbuf, lg, m_ref, s_ref, p_ref, stats, got,
           x_send, x_recv, wl_sem, wy_send, wy_recv, wp_send, wp_recv, st_send, st_recv):
    ny, nx, nz, chips, rows = plan.ny, plan.nx, plan.nz, plan.chips, plan.rows
    dp, vocab = lax.axis_index("dp"), lax.axis_index("vocab")
    y, core = dp // 2, dp % 2
    z, x = vocab // nx, vocab % nx
    me = vocab * ny + y
    model = lat_ref.shape[2]
    first_width = max(model // LANES // 7, 1) * LANES
    depth, cw = plan.depth, plan.cw

    def chip_device(b):
        return {"dp": (b % ny) * 2 + core, "vocab": b // ny}

    partner = {"dp": y * 2 + (1 - core), "vocab": vocab}

    base = pl.multiple_of(me * rows, rows)
    if rows != plan.per_dev:
        xbuf[pl.ds(base, rows), :] = jnp.zeros((rows, model), jnp.bfloat16)
    xbuf[pl.ds(base, plan.per_dev), :] = lat_ref[rank_ref[dp, 0]]

    barrier = pltpu.get_barrier_semaphore()

    @pl.loop(1, chips)
    def _(k):
        pl.semaphore_signal(barrier, inc=1, device_id=chip_device((me + k) % chips), device_id_type=MESH)

    pl.semaphore_signal(barrier, inc=1, device_id=partner, device_id_type=MESH)

    def w_rows(d):
        return pl.ds(pl.multiple_of(d * depth, depth), depth)

    def w_cols(j):
        return pl.ds(j * cw, cw)

    def window(y_at, j):
        return pl.ds(pl.multiple_of(plan.start(y_at) + j * cw, LANES), cw)

    locals_ = [
        pltpu.make_async_copy(w_ref.at[:, window(y, j)], wbuf.at[w_rows(dp), w_cols(j)], wl_sem.at[j])
        for j in range(plan.chunks)
    ]
    for copy in locals_:
        copy.start()
    pl.semaphore_wait(barrier, chips)

    def x_slice(flow, b):
        cols = pl.ds(0, first_width) if flow == 0 else pl.ds(first_width, model - first_width)
        return xbuf.at[pl.ds(pl.multiple_of(b * rows, rows), plan.sent_rows), cols]

    def chip(iy, ix, iz):
        return (iz * nx + ix) * ny + iy

    spot = {"y": (y, ny), "x": (x, nx), "z": (z, nz)}

    sends = []

    def x_copy(flow, b, axis, step, slot):
        to = {name: at for name, (at, _) in spot.items()}
        to[axis] = to[axis] + step
        return pltpu.make_async_remote_copy(
            src_ref=x_slice(flow, b), dst_ref=x_slice(flow, b), send_sem=x_send.at[slot], recv_sem=x_recv.at[flow, b],
            device_id={"dp": to["y"] * 2 + core, "vocab": to["z"] * nx + to["x"]}, device_id_type=MESH,
        )

    def send(flow, b, axis, step, here):
        copy = x_copy(flow, b, axis, step, len(sends))
        sends.append((copy, here))
        if here is None:
            copy.start()
        else:
            pl.when(here)(copy.start)

    def spread(flow, b, axis):
        at, n = spot[axis]
        if n == 2:
            send(flow, b, axis, 1 - 2 * at, None)
        elif n > 2:
            send(flow, b, axis, 1, at + 1 < n)
            send(flow, b, axis, -1, at > 0)

    def onward(flow, b, axis, origin):
        at, n = spot[axis]
        if n > 2:
            step = jnp.where(origin < at, 1, -1)
            send(flow, b, axis, step, jnp.logical_and(at + step >= 0, at + step < n))

    def arrived(flow, b):
        x_copy(flow, b, "y", 0, 0).wait_recv()

    def wy_copy(k, j):
        y_to = lax.rem(y + k, ny)
        return pltpu.make_async_remote_copy(
            src_ref=w_ref.at[:, window(y_to, j)], dst_ref=wbuf.at[w_rows(dp), w_cols(j)],
            send_sem=wy_send.at[k, j], recv_sem=wy_recv.at[k, j],
            device_id={"dp": y_to * 2 + core, "vocab": vocab}, device_id_type=MESH,
        )

    def wp_copy(k, j):
        d = lax.rem(y - k + ny, ny) * 2 + core
        place = wbuf.at[w_rows(d), w_cols(j)]
        return pltpu.make_async_remote_copy(
            src_ref=w_ref.at[:, window(y, j)] if k == 0 else place, dst_ref=place,
            send_sem=wp_send.at[k, j], recv_sem=wp_recv.at[k, j],
            device_id=partner, device_id_type=MESH,
        )

    started = []
    for axis in ("y", "x", "z"):
        for flow in (1, 0):
            spread(flow, me, axis)
    for j in range(plan.chunks):
        for k in range(1, ny):
            copy = wy_copy(k, j)
            copy.start()
            started.append(copy)
    for j in range(plan.chunks):
        copy = wp_copy(0, j)
        copy.start()
        started.append(copy)

    def forward_w(j):
        for k in range(1, ny):
            wy_copy(k, j).wait_recv()
            copy = wp_copy(k, j)
            copy.start()
            started.append(copy)

    src = {
        axis: [spot[axis][0]] + [source(*spot[axis], k) for k in range(1, spot[axis][1])] for axis in spot
    }

    def y_items():
        for iy in src["y"][1:]:
            for flow in (1, 0):
                b = chip(iy, x, z)
                arrived(flow, b)
                onward(flow, b, "y", iy)
                for axis in ("x", "z"):
                    spread(flow, b, axis)

    def first_x_items():
        for ix in src["x"][1:]:
            for iy in src["y"]:
                b = chip(iy, ix, z)
                arrived(0, b)
                onward(0, b, "x", ix)
                spread(0, b, "z")

    def first_z_items(k):
        iz = src["z"][k]
        for ix in src["x"]:
            for iy in src["y"]:
                b = chip(iy, ix, iz)
                arrived(0, b)
                onward(0, b, "z", iz)

    def second_z_items(k):
        iz = src["z"][k]
        for iy in src["y"]:
            b = chip(iy, x, iz)
            arrived(1, b)
            onward(1, b, "z", iz)
            spread(1, b, "x")

    def second_x_items(k):
        iz = src["z"][k]
        for ix in src["x"][1:]:
            for iy in src["y"]:
                b = chip(iy, ix, iz)
                arrived(1, b)
                onward(1, b, "x", ix)

    lane = lax.broadcasted_iota(jnp.int32, (1, LANES), 1)
    repeated = y * plan.own_tiles * LANES - plan.start(y)
    m_tile = plan.m_tile

    def score(k, low, high):
        top = pl.multiple_of(src["z"][k] * m_tile, m_tile)

        @pl.loop(low, high)
        def _(j):
            start = pl.multiple_of(j * cw, cw)
            lg[...] = jnp.dot(
                xbuf[pl.ds(top, m_tile), :], wbuf[:, pl.ds(start, cw)], preferred_element_type=jnp.float32
            )
            columns = [lane + (start + c * LANES) for c in range(cw // LANES)]
            own = [at >= repeated for at in columns]
            columns = [jnp.where(mine, at, -(2**30)) for mine, at in zip(own, columns)]

            @pl.loop(0, m_tile // 32, unroll=2)
            def _(r):
                here = pl.ds(pl.multiple_of(r * 32, 32), 32)
                there = pl.ds(pl.multiple_of(top + r * 32, 32), 32)
                parts = [lg[here, pl.ds(c * LANES, LANES)] for c in range(cw // LANES)]
                before = m_ref[there, :]
                now = before
                for part in parts:
                    now = jnp.maximum(now, part)
                total = s_ref[there, :] * jnp.exp(before - now)
                picked = p_ref[there, :]
                ids = ids_ref[there, :]
                for c, part in enumerate(parts):
                    total = total + jnp.where(own[c], jnp.exp(part - now), 0.0)
                    picked = picked + jnp.where(columns[c] == ids, part, 0.0)
                m_ref[there, :] = now
                s_ref[there, :] = total
                p_ref[there, :] = picked

    def w_ready(j):
        forward_w(j)
        locals_[j].wait()
        for k in range(ny):
            wp_copy(k, j).wait_recv()

    m_ref[...] = jnp.full(m_ref.shape, -jnp.inf, jnp.float32)
    s_ref[...] = jnp.zeros(s_ref.shape, jnp.float32)
    p_ref[...] = jnp.zeros(p_ref.shape, jnp.float32)
    y_items()
    first_x_items()
    if nz > 1:
        second_z_items(1)
    second_x_items(0)
    done_w = 0
    for k in range(1, nz):
        if k + 1 < nz:
            second_z_items(k + 1)
        if k == nz - 1:
            break
        first_z_items(k)
        second_x_items(k)
        until = plan.chunks * (k + 1) // nz
        for j in range(done_w, until):
            w_ready(j)
        for t in range(k):
            score(t, done_w, until)
        score(k, 0, until)
        done_w = until
    for j in range(done_w, plan.chunks):
        w_ready(j)
        for t in range(nz - 1):
            score(t, j, j + 1)
    if nz > 1:
        first_z_items(nz - 1)
        second_x_items(nz - 1)
    score(nz - 1, 0, plan.chunks)

    for g in range(plan.tokens // LANES):
        here = pl.ds(g * LANES, LANES)
        m = m_ref[here, :]
        top = jnp.max(m, axis=1, keepdims=True)
        total = jnp.sum(s_ref[here, :] * jnp.exp(m - top), axis=1, keepdims=True)
        picked = jnp.sum(p_ref[here, :], axis=1, keepdims=True)
        both = jnp.where(lane == 0, top, jnp.where(lane == 1, total, picked))
        stats[g] = both.T[:8, :]

    per_group = LANES // rows

    def st_copy(k):
        b = lax.rem(me + k, chips)
        return pltpu.make_async_remote_copy(
            src_ref=stats.at[b // per_group], dst_ref=got.at[k], send_sem=st_send, recv_sem=st_recv,
            device_id=chip_device(b), device_id_type=MESH,
        )

    @pl.loop(1, chips)
    def _(k):
        st_copy(k).start()

    got[0] = stats[me // per_group]
    for copy in started:
        copy.wait_send()
    for copy, here in sends:
        if here is None:
            copy.wait_send()
        else:
            pl.when(here)(copy.wait_send)
    others = got.at[pl.ds(1, chips - 1)]
    pltpu.make_async_copy(others, others, st_send).wait()
    pltpu.make_async_copy(others, others, st_recv).wait()
    top = got[0][0:1, :]
    for b in range(1, chips):
        top = jnp.maximum(top, got[b][0:1, :])
    total = jnp.zeros_like(top)
    picked = jnp.zeros_like(top)
    for b in range(chips):
        total = total + got[b][1:2, :] * jnp.exp(got[b][0:1, :] - top)
        picked = picked + got[b][2:3, :]
    result = picked - (top + jnp.log(total))
    place = lax.rem(me, per_group)
    value = result[:, : plan.per_dev]
    for c in range(1, per_group):
        value = jnp.where(place == c, result[:, c * rows : c * rows + plan.per_dev], value)
    out_ref[...] = value


def per_device(latent_activations, drawn_token_ids, retained_ranking, unembedding_matrix):
    depth, width = unembedding_matrix.shape
    n_dp, n_vocab = lax.axis_size("dp"), lax.axis_size("vocab")
    per_dev = latent_activations.shape[1]
    plan = Plan(n_dp, n_vocab, per_dev, width, depth)
    dp, vocab = lax.axis_index("dp"), lax.axis_index("vocab")
    ids = drawn_token_ids.reshape(n_dp, BATCH_PROPOSALS, n_vocab * per_dev)
    ids = jnp.where(retained_ranking[:, :1] == 0, ids[:, 0], ids[:, 1])
    ids = ids.reshape(plan.ny, 2, n_vocab, per_dev)
    ids = jnp.where(dp % 2 == 0, ids[:, 0], ids[:, 1]).transpose(1, 0, 2)
    ids = ids - (vocab * width + plan.start(dp // 2))
    ids = jnp.pad(ids, ((0, 0), (0, 0), (0, plan.rows - per_dev)), constant_values=-1)
    ids = ids.reshape(plan.tokens, 1)
    dma, vmem = pltpu.SemaphoreType.DMA, pltpu.VMEM
    model = depth * n_dp
    return pl.pallas_call(
        functools.partial(kernel, plan),
        out_shape=jax.ShapeDtypeStruct((1, per_dev), jnp.float32),
        in_specs=[
            pl.BlockSpec(memory_space=pltpu.SMEM),
            pl.BlockSpec(memory_space=vmem),
            pl.BlockSpec(memory_space=vmem),
            pl.BlockSpec(memory_space=pl.ANY),
        ],
        out_specs=pl.BlockSpec(memory_space=vmem),
        scratch_shapes=[
            vmem((plan.tokens, model), jnp.bfloat16),
            vmem((model, plan.cols), jnp.bfloat16),
            vmem((plan.m_tile, plan.cw), jnp.float32),
            vmem((plan.tokens, LANES), jnp.float32),
            vmem((plan.tokens, LANES), jnp.float32),
            vmem((plan.tokens, LANES), jnp.float32),
            vmem((plan.tokens // LANES, 8, LANES), jnp.float32),
            vmem((plan.chips, 8, LANES), jnp.float32),
            dma((plan.x_sends(),)), dma((2, plan.chips)),
            dma((plan.chunks,)),
            dma((plan.ny, plan.chunks)), dma((plan.ny, plan.chunks)),
            dma((plan.ny, plan.chunks)), dma((plan.ny, plan.chunks)),
            dma, dma,
        ],
        compiler_params=pltpu.CompilerParams(
            collective_id=0, has_side_effects=True, vmem_limit_bytes=56 * 2**20
        ),
        name="score",
    )(retained_ranking, latent_activations, ids, unembedding_matrix)


def solution(mesh):
    return jax.shard_map(
        per_device,
        mesh=mesh,
        in_specs=(P("dp", "vocab", None), P(), P(), P("dp", "vocab")),
        out_specs=P("dp", "vocab"),
        check_vma=False,
    )
```
